32 devices in a mesh: stn: 8 (over z, x), pts: 2 (over core), freq: 2 (over y).
Axes of the slice: x: 2, y: 2, z: 4, core: 2. Of those that a mesh axis runs over, the one named last changes fastest.
Arguments:
- greens: bfloat16 [2, 4, 2048, 4096], P(None, 'freq', 'stn', 'pts'), may hold values from -6 to 6
- noise_weights: bfloat16 [2, 4, 2048, 2048], P(None, 'freq', 'stn'), may hold values from -12 to 12, as said below
Outputs:
- kernel: float32 [4096], P('pts')
The draws below stay inside these ranges and needn't reach their ends.
Inputs may be any that keep to these rules, and one draw needn't show every extreme that they name: For every frequency, noise_weights[0] is symmetric and noise_weights[1] antisymmetric in the two station dimensions, so each frequency's matrix is Hermitian.
All inputs are finite; a program needn't handle non-finite values. Where the reference program divides by a largest or mean magnitude, that divisor is 1e-20 or more.
Results may differ from the reference program's by a relative error of at most 0.0003.
Values may be sent and summed in bfloat16 or wider, within the bound.
No kernel may reach another device: no remote copies, remote signals or barrier semaphores. Data moves between devices by JAX's collectives and lax.ppermute only.
A program may use at most 192 MiB of HBM per device.

```python
import jax
import jax.numpy as jnp
from jax import lax

S = 2048
F = 4
P_SIZE = 4096


def draw_noise_weights(key, part):
    base = jax.random.fold_in(key, 11)
    key_real, key_imag = jax.random.split(base, 2)
    rough_real = jax.random.truncated_normal(key_real, -4.0, 4.0, (F, S, S), jnp.float32) * 0.5
    rough_imag = jax.random.truncated_normal(key_imag, -4.0, 4.0, (F, S, S), jnp.float32) * 0.5
    symmetric = (rough_real + jnp.swapaxes(rough_real, 1, 2)) * 0.7071
    antisymmetric = (rough_imag - jnp.swapaxes(rough_imag, 1, 2)) * 0.7071
    return jnp.stack([symmetric, antisymmetric]).astype(jnp.bfloat16)


def levels(own_key, shape, shards, least, high):
    def one(position, blocks):
        steps = jax.random.uniform(jax.random.fold_in(jax.random.fold_in(own_key, 6), position), (blocks,), jnp.float32, least / len(shards), high / len(shards))
        return jnp.repeat(jnp.exp(steps), shape[position] // blocks).reshape((-1,) + (1,) * (len(shape) - position - 1))

    factor_of = one(*shards[0])
    for cut in shards[1:]:
        factor_of = factor_of * one(*cut)
    return factor_of


def noise(key, dims, deviation, most, pieces=(), kind=jnp.bfloat16):
    level = levels(key, dims, pieces, -0.22, 0.18) if pieces else 1.0
    result = jax.random.normal(key, dims, jnp.float32) * deviation * level
    return jnp.minimum(jnp.maximum(result, -most), most).astype(kind)


def setup_inputs(seed: int = 0) -> dict:
    seeds = jax.random.split(jax.random.key(seed), 3)
    greens = noise(seeds[0], (2, F, S, P_SIZE), 1.0, 6.0, ((1, 2), (2, 8), (3, 2)))
    noise_weights = draw_noise_weights(jax.random.fold_in(seeds[2], 71), 0)
    return {"greens": greens, "noise_weights": noise_weights}


def per_frequency(operands):
    green_block, weight_block = operands
    product_real = jnp.dot(weight_block[0], green_block[0], preferred_element_type=jnp.float32) - jnp.dot(weight_block[1], green_block[1], preferred_element_type=jnp.float32)
    product_imag = jnp.dot(weight_block[0], green_block[1], preferred_element_type=jnp.float32) + jnp.dot(weight_block[1], green_block[0], preferred_element_type=jnp.float32)
    green_real = green_block[0].astype(jnp.float32)
    green_imag = green_block[1].astype(jnp.float32)
    return jnp.sum(green_real * product_real + green_imag * product_imag, axis=0)


def reference(greens, noise_weights):
    stacked = lax.map(per_frequency, (jnp.moveaxis(greens, 1, 0), jnp.moveaxis(noise_weights, 1, 0)))
    raw_kernel = jnp.sum(stacked, axis=0) / S
    largest = jnp.max(jnp.abs(raw_kernel))
    return raw_kernel / (largest + 1e-6)
```

```python
import jax
import jax.numpy as jnp
from jax import lax
from jax.sharding import PartitionSpec as P


def ring_body(greens, noise_weights):
    station_rows = greens.shape[2]
    stations = noise_weights.shape[3]
    device_index = lax.axis_index("stn")
    cycle_length = lax.axis_size("stn")
    negated = -noise_weights[1]
    mixing = jnp.stack(
        [jnp.stack([noise_weights[0], negated]), jnp.stack([noise_weights[1], noise_weights[0]])]
    )

    def block_product(columns_start, arriving):
        weights_block = lax.dynamic_slice_in_dim(mixing, columns_start, station_rows, 4)
        return jnp.einsum(
            "ocfin,cfnx->ofix", weights_block, arriving, preferred_element_type=jnp.float32
        )

    summed = block_product(device_index * station_rows, greens)
    current = greens
    for offset in range(1, cycle_length):
        current = lax.ppermute(
            current, "stn", [(i, (i - 1) % cycle_length) for i in range(cycle_length)]
        )
        source = (device_index + offset) % cycle_length
        summed = summed + block_product(source * station_rows, current)
    parts = greens.astype(jnp.float32) * summed
    raw = lax.psum(jnp.sum(parts, axis=(0, 1, 2)) / stations, ("stn", "freq"))
    return raw / (lax.pmax(jnp.max(jnp.abs(raw)), "pts") + 1e-6)


def dot(lhs, rhs, lhs_dims, rhs_dims, batch=((), ())):
    return lax.dot_general(
        lhs, rhs, ((lhs_dims, rhs_dims), batch), preferred_element_type=jnp.float32
    )


def own_blocks(greens, noise_weights, block):
    freqs, rows = greens.shape[1:3]
    diagonal = lax.dynamic_slice_in_dim(noise_weights, block * rows, rows, 3)
    total = 0.0
    for f in range(freqs):
        real, imag = greens[0, f], greens[1, f]
        a, b = diagonal[0, f], diagonal[1, f]
        real32, imag32 = real.astype(jnp.float32), imag.astype(jnp.float32)
        total = total + jnp.sum(
            real32 * dot(a, real, (1,), (0,))
            + imag32 * (dot(a, imag, (1,), (0,)) + 2.0 * dot(b, real, (1,), (0,))),
            axis=0,
        )
    return total


def split_body(greens, noise_weights):
    size = lax.axis_size("stn")
    freqs, rows, points = greens.shape[1:]
    stations = noise_weights.shape[3]
    group = size // freqs
    half = group * rows
    width = points // group
    near = group // 2
    index = lax.axis_index("stn")
    mine, k = index // group, index % group
    part = lax.axis_index("pts")

    def send(x, offset):
        return lax.ppermute(x, "stn", [(i, i ^ offset) for i in range(size)])

    component = lax.dynamic_index_in_dim(noise_weights, part, 0, keepdims=False)

    def later_blocks(f):
        rows_f = lax.dynamic_index_in_dim(component, f, 0, keepdims=False)
        return jnp.concatenate(
            [
                lax.dynamic_slice_in_dim(rows_f, (mine * group + (k + j) % group) * rows, rows, 1)
                for j in range(1, near + 1)
            ],
            axis=1,
        )

    other_half_blocks = send(later_blocks(1 - mine), group)
    own_rows = lax.dynamic_index_in_dim(component, mine, 0, keepdims=False)
    across = lax.dynamic_slice_in_dim(own_rows, (1 - mine) * half, half, 1)
    unit = jnp.concatenate([across, later_blocks(mine)], axis=1)

    def chunk_for(target):
        return lax.dynamic_slice(
            greens,
            (0, target // group, 0, (target % group) * width),
            (2, 1, rows, width),
        )[:, 0]

    def exchange(h, j):
        perm = [(i, (i // group ^ h) * group + (i % group + j) % group) for i in range(size)]
        target = (mine ^ h) * group + (k + j) % group
        return lax.ppermute(chunk_for(target), "stn", perm)

    units, later = {0: unit}, {0: other_half_blocks}
    far, own = {}, {0: chunk_for(index)}
    order = list(range(1, group)) + [0]
    far[order[0]] = exchange(1, order[0])

    def spread(pieces):
        bit = group // 2
        while bit:
            pieces.update({o ^ bit: send(x, bit) for o, x in pieces.items()})
            bit //= 2

    spread(units)
    spread(later)
    for j in range(1, group):
        own[j] = exchange(0, j)
    for j in order[1:]:
        far[j] = exchange(1, j)

    both = jnp.stack([jnp.concatenate([units[o], later[o]], axis=1) for o in range(group)])
    both = jnp.stack(
        [
            lax.dynamic_index_in_dim(both, k ^ ((k + t) % group), 0, keepdims=False)
            for t in range(group)
        ]
    )
    crossed = lax.ppermute(both, "pts", [(0, 1), (1, 0)])
    is_real = part == 0
    weights = jnp.stack([jnp.where(is_real, both, crossed), jnp.where(is_real, crossed, both)])
    w_across = weights[..., :half]
    blocked = (2, group, rows, near, rows)
    w_own = weights[..., half : half + near * rows].reshape(blocked)
    w_far = weights[..., half + near * rows :].reshape(blocked)

    g_own = jnp.stack([own[(-t) % group] for t in range(group)], axis=1)

    def turned(g):
        return jnp.concatenate([g, jnp.stack([g[1], -g[0]])], axis=-1)

    def forward(w, g):
        ahead = jnp.stack(
            [g * (1 if j == near and 2 * near == group else 2) for j in range(1, near + 1)]
        )
        ahead = jnp.stack(
            [jnp.roll(ahead[j], -(j + 1), axis=1) for j in range(near)], axis=2
        )
        signed = jnp.stack([ahead[0], -ahead[1]])
        swapped = jnp.stack([ahead[1], ahead[0]])
        real = dot(w, signed, (0, 3, 4), (0, 2, 3), ((1,), (1,)))
        imag = dot(w, swapped, (0, 3, 4), (0, 2, 3), ((1,), (1,)))
        return jnp.stack([real, imag])

    reach = dot(w_across, turned(g_own), (0, 1, 2), (0, 1, 2))
    reach = reach.reshape(group, rows, 2, width)

    def reach_of(t):
        block = lax.dynamic_index_in_dim(reach, (k + t) % group, 0, keepdims=False)
        return 2.0 * jnp.moveaxis(block, 1, 0)

    own_sum = jnp.sum(g_own.astype(jnp.float32) * forward(w_own, g_own), axis=(0, 1, 2))

    g_far = jnp.stack(
        [jnp.zeros_like(own[0])] + [far[(-t) % group] for t in range(1, group)], axis=1
    )
    u_far = forward(w_far, g_far)
    last = reach_of(0) + u_far[:, 0]
    for j in range(1, near + 1):
        scale = 1.0 if 2 * j == group else 2.0
        back = dot(
            w_far[:, group - j, :, j - 1], turned(g_far[:, group - j]), (0, 1), (0, 1)
        )
        last = last + scale * jnp.moveaxis(back.reshape(rows, 2, width), 1, 0)
    rest = sum(
        jnp.sum(far[(-t) % group].astype(jnp.float32) * (reach_of(t) + u_far[:, t]), axis=(0, 1))
        for t in range(1, group)
    )
    home = own_blocks(greens, noise_weights, index)
    ready = own_sum + rest
    slice_sum = ready + jnp.sum(far[0].astype(jnp.float32) * last, axis=(0, 1))
    start = k * width
    piece = lax.dynamic_slice_in_dim(home, start, width, 0) + slice_sum
    raw = lax.dynamic_update_slice_in_dim(home, piece, start, 0) / stations

    bit = 1
    while bit < size:
        raw = raw + send(raw, bit)
        bit *= 2
    raw = raw + lax.ppermute(raw, "freq", [(0, 1), (1, 0)])
    largest = jnp.max(jnp.abs(raw)).reshape(1)
    largest = jnp.maximum(largest, lax.ppermute(largest, "pts", [(0, 1), (1, 0)]))
    return raw / (largest + 1e-6)


def fits(mesh, greens):
    sizes = mesh.shape
    freqs = greens.shape[1] // sizes["freq"]
    group = sizes["stn"] // 2
    return (
        freqs == 2
        and sizes["pts"] == 2
        and sizes["freq"] == 2
        and group >= 2
        and sizes["stn"] & (sizes["stn"] - 1) == 0
        and (greens.shape[3] // sizes["pts"]) % group == 0
    )


def solution(mesh):
    in_specs = (P(None, "freq", "stn", "pts"), P(None, "freq", "stn", None))

    def step(greens, noise_weights):
        body = split_body if fits(mesh, greens) else ring_body
        return jax.shard_map(
            body, mesh=mesh, in_specs=in_specs, out_specs=P("pts"), check_vma=False
        )(greens, noise_weights)

    return step
```
